32 devices in a mesh: dp: 8 (over y, x, core), expert: 4 (over z).
Axes of the slice: x: 2, y: 2, z: 4, core: 2. Of those that a mesh axis runs over, the one named last changes fastest.
Arguments:
- tokens: bfloat16 [4096, 1024], P(('dp', 'expert')), may hold values from -24 to 24
- route_first: int32 [4096, 1], P(('dp', 'expert')), may hold values from 0 to 1; in each aligned block of 128 rows (0 to 127, 128 to 255, ...) at most 68 rows name the same one
- route_second: int32 [4096, 1], P(('dp', 'expert')), may hold values from 0 to 1; in each aligned block of 128 rows (0 to 127, 128 to 255, ...) at most 68 rows name the same one
- up_first: bfloat16 [4, 1024, 2048], P('expert', 'dp'), may hold values from -0.1875 to 0.1875
- down_first: bfloat16 [4, 2048, 1024], P('expert', 'dp'), may hold values from -0.09375 to 0.09375
- up_second: bfloat16 [4, 1024, 2048], P('expert', 'dp'), may hold values from -0.1875 to 0.1875
- down_second: bfloat16 [4, 2048, 1024], P('expert', 'dp'), may hold values from -0.09375 to 0.09375
- cotangent: bfloat16 [4096, 1024], P(('dp', 'expert')), may hold values from -6 to 6
Outputs:
- layer_out: bfloat16 [4096, 1024], P(('dp', 'expert'))
- grad_tokens: bfloat16 [4096, 1024], P(('dp', 'expert'))
- grad_up_first: float32 [4, 1024, 2048], P('expert', 'dp')
- grad_down_first: float32 [4, 2048, 1024], P('expert', 'dp')
- grad_up_second: float32 [4, 1024, 2048], P('expert', 'dp')
- grad_down_second: float32 [4, 2048, 1024], P('expert', 'dp')
The draws below stay inside these ranges and needn't reach their ends.
Inputs may be any that keep to these rules, and one draw needn't show every extreme that they name: `route_first`: in each aligned block of 128 rows (the rows of one device) no expert id appears more than 68 times, and in every draw some expert appears exactly 68 times in some block. `route_second`: in each aligned block of 128 rows (the rows of one device) no expert id appears more than 68 times, and in every draw some expert appears exactly 68 times in some block.
All inputs are finite; a program needn't handle non-finite values.
Results may differ from the reference program's by a relative error of at most 0.025.
Values may be sent and summed in bfloat16 or wider, within the bound.
A program may use at most 128 MiB of HBM per device.

```python
import math
import jax
import jax.numpy as jnp
import numpy as np
from jax import lax

D = 1024
FF = 4096
TOK_DEV = 128
TOKENS = 4096
EXP_A = 2
HID_A = 2048
CAP_A = 68
EXP_B = 2
HID_B = 2048
CAP_B = 68
N_DP = 8
N_EXPERT = 4


def draw_tokens(key, part):
    keys = jax.random.split(jax.random.fold_in(key, 11), 3)
    row_scale = jnp.exp(jax.random.uniform(keys[0], (TOKENS, 1), jnp.float32, jnp.log(0.3), jnp.log(3.0)))
    column_scale = jnp.exp(jax.random.uniform(keys[1], (1, D), jnp.float32, jnp.log(0.5), jnp.log(2.0)))
    values = jnp.clip(jax.random.normal(keys[2], (TOKENS, D), jnp.float32), -4.0, 4.0)
    return (values * row_scale * column_scale).astype(jnp.bfloat16)


def shard_levels(key, dims, cuts, smallest, largest):
    def one(axis_at, blocks):
        heights = jax.random.uniform(jax.random.fold_in(jax.random.fold_in(key, 6), axis_at), (blocks,), jnp.float32, smallest / len(cuts), largest / len(cuts))
        return jnp.repeat(jnp.exp(heights), dims[axis_at] // blocks).reshape((-1,) + (1,) * (len(dims) - axis_at - 1))

    loudness = one(*cuts[0])
    for cut in cuts[1:]:
        loudness = loudness * one(*cut)
    return loudness


def assign_block(own_key, own, number, rows, count, top, bound, lean):
    sequence = jax.random.permutation(own_key, count)
    heavy_load, usual = portions_of(count, rows * top, bound, lean, True), portions_of(count, rows * top, bound, lean, False)
    places = jnp.arange(count)

    def named(tallies, offset_by):
        used = int((tallies > 0).sum())
        fixed = max(1, used // 4)
        shifted = fixed + (places - fixed + offset_by * (used - fixed)) % max(1, count - fixed)
        return jnp.zeros((count,), jnp.int32).at[sequence[jnp.where(places < fixed, places, shifted)]].set(jnp.asarray(tallies, jnp.int32))

    tallies = jnp.where(number % 4 == 0, named(heavy_load, number // 4), named(usual, number - number // 4 - 1))
    mixed = jax.random.permutation(jax.random.fold_in(own, 3), count)
    giver, receiver = mixed[0:count // 2 * 2:2], mixed[1:count // 2 * 2:2]
    room = jnp.minimum(tallies[giver] - 1, bound - tallies[receiver]) // 2
    room = jnp.where((giver == sequence[0]) | (receiver == sequence[0]) | (tallies[receiver] == 0), 0, jnp.maximum(room, 0))
    shifted = jax.random.randint(jax.random.fold_in(own, 4), (count // 2,), 0, 1 << 20) % (room + 1)
    tallies = tallies.at[giver].add(-shifted).at[receiver].add(shifted)
    members = jnp.searchsorted(jnp.cumsum(tallies), jnp.arange(rows * top), side="right").astype(jnp.int32)
    listing = members.reshape(top, rows).T
    listing = listing[jax.random.permutation(jax.random.fold_in(own, 1), rows)]
    offset_by = jax.random.randint(jax.random.fold_in(own, 2), (rows, 1), 0, top)
    return jnp.take_along_axis(listing, (jnp.arange(top)[None, :] + offset_by) % top, axis=1)


def portions_of(number_of, total, bound, skew, full):
    loads = [(1 << 20) // math.isqrt(standing ** skew) + 1 for standing in range(1, number_of + 1)]
    largest = bound if full else min(bound, max(-(-total // number_of), total * loads[0] // sum(loads)))
    least = 1 if total - largest >= number_of - 1 else 0
    holding, rest = [largest] + [least] * (number_of - 1), total - largest - least * (number_of - 1)
    while rest > 0:
        movable = [i for i in range(1, number_of) if holding[i] < largest] or [i for i in range(1, number_of) if holding[i] < bound]
        pool, left = sum([loads[i] for i in movable]), rest
        for i in movable:
            addition = min(bound - holding[i], max(1, left * loads[i] // pool), rest)
            holding[i] = holding[i] + addition
            rest = rest - addition
    return np.array(holding)


def centred(rng, extent, scale, bound, cuts=(), kind=jnp.bfloat16):
    drawn = scale * jax.random.normal(rng, extent, jnp.float32)
    if cuts:
        drawn = drawn * shard_levels(rng, extent, cuts, -0.22, 0.18)
    return jnp.clip(drawn, -bound, bound).astype(kind)


def setup_inputs(seed: int = 0) -> dict:
    splits = jax.random.split(jax.random.key(seed), 9)
    tokens = draw_tokens(jax.random.fold_in(splits[8], 71), 0)
    route_first_keys = jax.random.split(jax.random.fold_in(splits[1], 1), TOKENS // TOK_DEV)
    route_first_turns = jax.random.permutation(jax.random.fold_in(splits[1], 3), TOKENS // TOK_DEV)
    route_first = jax.vmap(lambda own, number: assign_block(jax.random.fold_in(splits[1], 2), own, number, TOK_DEV, EXP_A, 1, CAP_A, 2))(route_first_keys, route_first_turns).reshape((TOKENS, 1))
    route_second_keys = jax.random.split(jax.random.fold_in(splits[2], 1), TOKENS // TOK_DEV)
    route_second_turns = jax.random.permutation(jax.random.fold_in(splits[2], 3), TOKENS // TOK_DEV)
    route_second = jax.vmap(lambda own, number: assign_block(jax.random.fold_in(splits[2], 2), own, number, TOK_DEV, EXP_B, 1, CAP_B, 2))(route_second_keys, route_second_turns).reshape((TOKENS, 1))
    up_first = centred(splits[3], (N_EXPERT, D, HID_A), D ** -0.5, 0.1875, ((0, 4), (1, 8)))
    down_first = centred(splits[4], (N_EXPERT, HID_A, D), FF ** -0.5, 0.09375, ((0, 4), (1, 8)))
    up_second = centred(splits[5], (N_EXPERT, D, HID_B), D ** -0.5, 0.1875, ((0, 4), (1, 8)))
    down_second = centred(splits[6], (N_EXPERT, HID_B, D), FF ** -0.5, 0.09375, ((0, 4), (1, 8)))
    cotangent = centred(splits[7], (TOKENS, D), 1.0, 6.0, ((0, 32),))
    return dict(tokens=tokens, route_first=route_first, route_second=route_second, up_first=up_first, down_first=down_first, up_second=up_second, down_second=down_second, cotangent=cotangent)


epsilon = 1e-06

def rms_normal(widened):
    return widened * lax.rsqrt(lax.optimization_barrier(jnp.mean(widened * widened, axis=-1, keepdims=True)) + epsilon)

def gelu_slope(pre_gelu):
    _, pullback = jax.vjp(jax.nn.gelu, pre_gelu)
    return pullback(jnp.ones_like(pre_gelu))[0]

def slot_places(route_ids, experts, capacity):
    expert_ids = route_ids[:, 0].reshape(-1, TOK_DEV)
    onehot = (expert_ids[:, :, None] == jnp.arange(experts, dtype=jnp.int32)[None, None, :]).astype(jnp.int32)
    earlier = jnp.cumsum(onehot, axis=1) - onehot
    return expert_ids * capacity + lax.optimization_barrier(jnp.sum(earlier * onehot, axis=2))

def spread(token_rows, places, experts, capacity):
    feature_count = token_rows.shape[1]
    blocks = token_rows.reshape(-1, TOK_DEV, feature_count)

    def place_block(block, block_places):
        return jnp.zeros((experts * capacity, feature_count), block.dtype).at[block_places].set(block)
    filled = jax.vmap(place_block)(blocks, places)
    return filled.reshape(N_DP, N_EXPERT, experts, capacity, feature_count)

def pick_rows(slot_table, block_places):
    return slot_table[block_places]

def collect(parts, places, experts):
    group_size = N_EXPERT // experts
    capacity = parts.shape[3]
    feature_count = parts.shape[4]
    summed = parts.astype(jnp.float32).reshape(experts, group_size, N_DP, N_EXPERT, capacity, feature_count).sum(axis=1)
    summed = jnp.transpose(summed, (1, 2, 0, 3, 4)).reshape(N_DP * N_EXPERT, experts * capacity, feature_count)
    picked = jax.vmap(pick_rows)(summed, places)
    return picked.reshape(-1, feature_count)

def column_inputs(buffers, column, group_size):
    return lax.dynamic_index_in_dim(buffers, column // group_size, axis=2, keepdims=False).astype(jnp.float32)

def layer_forward(token_rows, route_ids, up_full, down_full, experts, capacity):
    group_size = N_EXPERT // experts
    places = slot_places(route_ids, experts, capacity)
    widened = token_rows.astype(jnp.float32)
    normed = rms_normal(widened).astype(jnp.bfloat16)
    buffers = spread(normed, places, experts, capacity)

    def forward_column(column_args):
        column, up_one, down_one = column_args
        received = column_inputs(buffers, column, group_size)
        pre_gelu = jnp.einsum('abkd,dh->abkh', received, up_one.astype(jnp.float32))
        hidden = lax.optimization_barrier(jax.nn.gelu(pre_gelu).astype(jnp.bfloat16)).astype(jnp.float32)
        return jnp.einsum('abkh,hd->abkd', hidden, down_one.astype(jnp.float32)).astype(jnp.bfloat16)
    columns = jnp.arange(N_EXPERT, dtype=jnp.int32)
    parts = lax.map(forward_column, (columns, up_full, down_full))
    branch = collect(parts, places, experts)
    return ((widened + branch).astype(jnp.bfloat16), (widened, places, buffers))

def layer_backward(upstream, saved, up_full, down_full, experts, capacity):
    widened, places, buffers = saved
    group_size = N_EXPERT // experts
    arrivals = spread(upstream, places, experts, capacity)

    def backward_column(column_args):
        column, up_one, down_one = column_args
        received = column_inputs(buffers, column, group_size)
        arriving = column_inputs(arrivals, column, group_size)
        up_wide = up_one.astype(jnp.float32)
        down_wide = down_one.astype(jnp.float32)
        pre_gelu = jnp.einsum('abkd,dh->abkh', received, up_wide)
        hidden = lax.optimization_barrier(jax.nn.gelu(pre_gelu).astype(jnp.bfloat16)).astype(jnp.float32)
        grad_pre = (jnp.einsum('abkd,hd->abkh', arriving, down_wide) * gelu_slope(pre_gelu)).astype(jnp.bfloat16)
        grad_wide = lax.optimization_barrier(grad_pre).astype(jnp.float32)
        down_rows = jnp.einsum('abkh,abkd->ahd', hidden, arriving)
        grad_down = lax.optimization_barrier(down_rows.astype(jnp.bfloat16)).astype(jnp.float32).sum(axis=0)
        up_rows = jnp.einsum('abkd,abkh->adh', received, grad_wide)
        grad_up = lax.optimization_barrier(up_rows.astype(jnp.bfloat16)).astype(jnp.float32).sum(axis=0)
        grad_slots = jnp.einsum('abkh,dh->abkd', grad_wide, up_wide).astype(jnp.bfloat16)
        return (grad_up, grad_down, grad_slots)
    columns = jnp.arange(N_EXPERT, dtype=jnp.int32)
    grad_ups, grad_downs, slot_grads = lax.map(backward_column, (columns, up_full, down_full))
    grad_normed = collect(slot_grads, places, experts)
    _, pullback = jax.vjp(rms_normal, widened)
    grad_input = (upstream.astype(jnp.float32) + pullback(grad_normed)[0]).astype(jnp.bfloat16)
    return (grad_input, grad_ups, grad_downs)

def reference(tokens, route_first, route_second, up_first, down_first, up_second, down_second, cotangent):
    middle, first_saved = layer_forward(tokens, route_first, up_first, down_first, EXP_A, CAP_A)
    layer_out, second_saved = layer_forward(middle, route_second, up_second, down_second, EXP_B, CAP_B)
    grad_middle, grad_up_second, grad_down_second = layer_backward(cotangent, second_saved, up_second, down_second, EXP_B, CAP_B)
    grad_tokens, grad_up_first, grad_down_first = layer_backward(grad_middle, first_saved, up_first, down_first, EXP_A, CAP_A)
    return (layer_out, grad_tokens, grad_up_first, grad_down_first, grad_up_second, grad_down_second)
```

```python
import functools

import jax
import jax.numpy as jnp
from jax import lax
from jax.experimental import pallas as pl
from jax.experimental.pallas import tpu as pltpu
from jax.sharding import PartitionSpec as P

epsilon = 1e-06


def rms_normal(widened):
    return widened * lax.rsqrt(jnp.mean(widened * widened, axis=-1, keepdims=True) + epsilon)


def gelu_slope(pre_gelu):
    _, pullback = jax.vjp(jax.nn.gelu, pre_gelu)
    return pullback(jnp.ones_like(pre_gelu))[0]


def slot_places(route_ids, experts, capacity):
    expert_ids = route_ids[:, 0]
    onehot = (expert_ids[:, None] == jnp.arange(experts, dtype=jnp.int32)[None, :]).astype(
        jnp.int32
    )
    earlier = jnp.cumsum(onehot, axis=0) - onehot
    return expert_ids * capacity + jnp.sum(earlier * onehot, axis=1)


def to_slots(token_rows, places, slot_count):
    onehot_table = (places[None, :] == jnp.arange(slot_count, dtype=jnp.int32)[:, None]).astype(
        token_rows.dtype
    )
    return jnp.dot(onehot_table, token_rows, preferred_element_type=jnp.float32).astype(
        token_rows.dtype
    )


def from_slots(returned, places, experts):
    group_size = returned.shape[0] // experts
    feature_count = returned.shape[2]
    summed = (
        returned.reshape(experts, group_size, returned.shape[1], feature_count)
        .astype(jnp.float32)
        .sum(axis=1)
    )
    summed = summed.reshape(-1, feature_count)
    onehot_table = (
        places[:, None] == jnp.arange(summed.shape[0], dtype=jnp.int32)[None, :]
    ).astype(jnp.float32)
    return jnp.dot(
        onehot_table, summed, precision=lax.Precision.HIGHEST, preferred_element_type=jnp.float32
    )


VMEM_LIMIT = 48 * 1024 * 1024


def comm_kernel(gather_rows, scatter_rows, exchange_slots, *refs):
    n_gather, n_scatter, n_exchange = len(gather_rows), len(scatter_rows), len(exchange_slots)
    refs = list(refs)

    def take(count):
        taken = refs[:count]
        del refs[:count]
        return taken

    shards, grads, outgoing = take(n_gather), take(n_scatter), take(n_exchange)
    fulls, sums, received = take(n_gather), take(n_scatter), take(n_exchange)
    scatter_scratch = [take(8) for _ in range(n_scatter)]
    send_sems, recv_sems, local_sems = take(3)
    used = [0, 0]

    dp = lax.axis_index("dp")
    z = lax.axis_index("expert")
    z_count = lax.axis_size("expert")
    core = lax.rem(dp, 2)
    x_bit = lax.rem(lax.div(dp, 2), 2)
    y_bit = lax.div(dp, 4)
    twin = dp + 1 - 2 * core
    x_side = dp + 2 - 4 * x_bit
    y_side = dp + 4 - 8 * y_bit
    diagonal = x_side + 4 - 8 * y_bit

    barrier = pltpu.get_barrier_semaphore()
    peers = 0
    if n_gather or n_scatter:
        for side in (twin, x_side, y_side):
            pl.semaphore_signal(
                barrier, inc=1, device_id=(side, z), device_id_type=pl.DeviceIdType.MESH
            )
            peers += 1
    if n_exchange:
        for step in range(1, z_count):
            pl.semaphore_signal(
                barrier,
                inc=1,
                device_id=(dp, lax.rem(z + step, z_count)),
                device_id_type=pl.DeviceIdType.MESH,
            )
            peers += 1
    pl.semaphore_wait(barrier, peers)

    def send(source, target, to_dp, to_z):
        index = used[0]
        used[0] += 1
        copy = pltpu.make_async_remote_copy(
            src_ref=source,
            dst_ref=target,
            send_sem=send_sems.at[index],
            recv_sem=recv_sems.at[index],
            device_id=(to_dp, to_z),
            device_id_type=pl.DeviceIdType.MESH,
        )
        copy.start()
        return copy

    def keep(source, target):
        index = used[1]
        used[1] += 1
        copy = pltpu.make_async_copy(source, target, local_sems.at[index])
        copy.start()
        return copy

    remote, local = [], []
    swaps = []
    for grad, rows, scratch in zip(grads, scatter_rows, scatter_scratch):
        from_twin = scratch[0]
        swap = []
        for slot, owner in enumerate((diagonal, x_side, y_side, dp)):
            theirs = owner + 1 - 2 * core
            part = grad.at[pl.ds(pl.multiple_of(theirs * rows, rows), rows), :]
            swap.append(send(part, from_twin.at[slot], twin, z))
        swaps.append(swap)

    for source, target, slots in zip(outgoing, received, exchange_slots):
        for step in range(1, z_count):
            to_z = lax.rem(z + step, z_count)
            slot = lax.div(to_z * slots, z_count)
            remote.append(send(source.at[slot], target.at[z], dp, to_z))
        local.append(keep(source.at[lax.div(z * slots, z_count)], target.at[z]))

    def rows_of(ref, owner, rows, start=0, count=None):
        offset = pl.multiple_of(owner * rows + start, rows if count is None else count)
        return ref.at[pl.ds(offset, rows if count is None else count), :]

    firsts = []
    for shard, full, rows in zip(shards, fulls, gather_rows):
        mine = rows_of(full, dp, rows)
        firsts.append((send(shard, mine, x_side, z), send(shard, mine, y_side, z)))
        remote.append(send(shard, mine, twin, z))
        local.append(keep(shard, mine))

    diagonals = []
    for full, rows, (along_x, along_y) in zip(fulls, gather_rows, firsts):
        half = rows // 2
        along_x.wait_recv()
        part = rows_of(full, x_side, rows, 0, half)
        lower = send(part, part, y_side, z)
        part = rows_of(full, x_side, rows)
        remote.append(send(part, part, twin, z))
        along_y.wait_recv()
        part = rows_of(full, y_side, rows, half, half)
        upper = send(part, part, x_side, z)
        part = rows_of(full, y_side, rows)
        remote.append(send(part, part, twin, z))
        along_x.wait_send()
        along_y.wait_send()
        diagonals.append((lower, upper))
    for full, rows, (lower, upper) in zip(fulls, gather_rows, diagonals):
        half = rows // 2
        lower.wait_recv()
        part = rows_of(full, diagonal, rows, 0, half)
        remote.append(send(part, part, twin, z))
        upper.wait_recv()
        part = rows_of(full, diagonal, rows, half, half)
        remote.append(send(part, part, twin, z))
        lower.wait_send()
        upper.wait_send()

    def wide(ref):
        return ref[...].astype(jnp.float32)

    halves = []
    for grad, rows, scratch, swap in zip(grads, scatter_rows, scatter_scratch, swaps):
        from_twin, to_diagonal, to_x, to_y, via_x, via_y, from_x, from_y = scratch
        half = rows // 2
        swap[0].wait_recv()
        to_diagonal[...] = (
            wide(rows_of(grad, diagonal, rows)) + wide(from_twin.at[0])
        ).astype(jnp.bfloat16)
        swap[1].wait_recv()
        to_x[...] = (wide(rows_of(grad, x_side, rows)) + wide(from_twin.at[1])).astype(
            jnp.bfloat16
        )
        low, high = pl.ds(0, half), pl.ds(half, half)
        relay_x = send(to_diagonal.at[low, :], via_x, x_side, z)
        relay_y = send(to_diagonal.at[high, :], via_y, y_side, z)
        swap[2].wait_recv()
        to_y[...] = (wide(rows_of(grad, y_side, rows)) + wide(from_twin.at[2])).astype(
            jnp.bfloat16
        )
        direct_x = send(to_x.at[low, :], from_x.at[low, :], x_side, z)
        direct_y = send(to_y.at[high, :], from_y.at[high, :], y_side, z)
        swap[3].wait_recv()
        halves.append((relay_x, relay_y, direct_x, direct_y))
    finals = []
    for rows, scratch, (relay_x, relay_y, direct_x, direct_y) in zip(
        scatter_rows, scatter_scratch, halves
    ):
        from_twin, to_diagonal, to_x, to_y, via_x, via_y, from_x, from_y = scratch
        half = rows // 2
        low, high = pl.ds(0, half), pl.ds(half, half)
        relay_y.wait_recv()
        to_x[high, :] = (wide(to_x.at[high, :]) + wide(via_y)).astype(jnp.bfloat16)
        relay_x.wait_recv()
        to_y[low, :] = (wide(to_y.at[low, :]) + wide(via_x)).astype(jnp.bfloat16)
        last_x = send(to_x.at[high, :], from_x.at[high, :], x_side, z)
        last_y = send(to_y.at[low, :], from_y.at[low, :], y_side, z)
        finals.append((last_x, last_y))
    for grad, total, rows, scratch, swap, pieces, last in zip(
        grads, sums, scatter_rows, scatter_scratch, swaps, halves, finals
    ):
        from_twin, to_diagonal, to_x, to_y, via_x, via_y, from_x, from_y = scratch
        for copy in pieces[2:] + last:
            copy.wait_recv()
        total[...] = (
            wide(rows_of(grad, dp, rows)) + wide(from_twin.at[3]) + wide(from_x) + wide(from_y)
        )
        for copy in tuple(swap) + pieces + last:
            copy.wait_send()
    for copy in remote:
        copy.wait()
    for copy in local:
        copy.wait()


def communicate(collective_id, gathers=(), scatters=(), exchanges=()):
    ways = lax.axis_size("dp")
    z_count = lax.axis_size("expert")
    if ways != 8:
        fulls = [lax.all_gather(shard, "dp", axis=0, tiled=True) for shard in gathers]
        sums = [
            lax.psum_scatter(grad, "dp", scatter_dimension=0, tiled=True).astype(jnp.float32)
            for grad in scatters
        ]
        received = [
            lax.all_to_all(
                jnp.repeat(slots, z_count // slots.shape[0], axis=0),
                "expert",
                split_axis=0,
                concat_axis=0,
                tiled=True,
            )
            for slots in exchanges
        ]
        return (*fulls, *sums, *received)
    outs, out_specs, scratch = [], [], []
    for shard in gathers:
        outs.append(jax.ShapeDtypeStruct((ways * shard.shape[0], shard.shape[1]), shard.dtype))
        out_specs.append(pl.BlockSpec(memory_space=pl.ANY))
    for grad in scatters:
        rows, columns = grad.shape[0] // ways, grad.shape[1]
        outs.append(jax.ShapeDtypeStruct((rows, columns), jnp.float32))
        out_specs.append(pl.BlockSpec(memory_space=pltpu.VMEM))
        scratch.append(pltpu.VMEM((4, rows, columns), grad.dtype))
        for height in (rows, rows, rows, rows // 2, rows // 2, rows, rows):
            scratch.append(pltpu.VMEM((height, columns), grad.dtype))
    for slots in exchanges:
        outs.append(jax.ShapeDtypeStruct((z_count, *slots.shape[1:]), slots.dtype))
        out_specs.append(pl.BlockSpec(memory_space=pl.ANY))
    copies = 9 * len(gathers) + 10 * len(scatters) + (z_count - 1) * len(exchanges)
    scratch += [
        pltpu.SemaphoreType.DMA((copies,)),
        pltpu.SemaphoreType.DMA((copies,)),
        pltpu.SemaphoreType.DMA((max(len(gathers) + len(exchanges), 1),)),
    ]
    inputs = (*gathers, *scatters, *exchanges)
    return pl.pallas_call(
        functools.partial(
            comm_kernel,
            tuple(shard.shape[0] for shard in gathers),
            tuple(grad.shape[0] // ways for grad in scatters),
            tuple(slots.shape[0] for slots in exchanges),
        ),
        out_shape=tuple(outs),
        in_specs=[pl.BlockSpec(memory_space=pltpu.VMEM)] * len(inputs),
        out_specs=tuple(out_specs),
        scratch_shapes=scratch,
        compiler_params=pltpu.CompilerParams(
            collective_id=collective_id, has_side_effects=True, vmem_limit_bytes=VMEM_LIMIT
        ),
        name="comm_%d" % collective_id,
    )(*inputs)


def slotted(token_rows, places, experts, capacity):
    return to_slots(token_rows, places, experts * capacity).reshape(experts, capacity, -1)


def project_up(received, up_full):
    pre_gelu = jnp.einsum("skd,dh->skh", received, up_full, preferred_element_type=jnp.float32)
    return pre_gelu, jax.nn.gelu(pre_gelu).astype(jnp.bfloat16)


def project_down(hidden, down_full):
    return jnp.einsum("skh,hd->skd", hidden, down_full, preferred_element_type=jnp.float32).astype(
        jnp.bfloat16
    )


def layer_gradients(arriving, received, pre_gelu, hidden, up_full, down_full):
    grad_hidden = jnp.einsum("skd,hd->skh", arriving, down_full, preferred_element_type=jnp.float32)
    grad_pre = (grad_hidden * gelu_slope(pre_gelu)).astype(jnp.bfloat16)
    grad_down = jnp.einsum("skh,skd->hd", hidden, arriving, preferred_element_type=jnp.float32)
    grad_up = jnp.einsum("skd,skh->dh", received, grad_pre, preferred_element_type=jnp.float32)
    grad_slots = jnp.einsum(
        "skh,dh->skd", grad_pre, up_full, preferred_element_type=jnp.float32
    ).astype(jnp.bfloat16)
    return grad_up.astype(jnp.bfloat16), grad_down.astype(jnp.bfloat16), grad_slots


def grad_through_norm(upstream, widened, grad_normed):
    _, pullback = jax.vjp(rms_normal, widened)
    return (upstream.astype(jnp.float32) + pullback(grad_normed)[0]).astype(jnp.bfloat16)


def capacity_for(token_count, experts):
    return min(token_count, (token_count * 17 + 16 * experts - 1) // (16 * experts))


def local(
    tokens, route_first, route_second, up_first, down_first, up_second, down_second, cotangent
):
    expert_devices = lax.axis_size("expert")
    token_count = tokens.shape[0]
    experts_first = max(expert_devices // 4, 2)
    experts_second = max(expert_devices // 2, 2)
    cap_first = capacity_for(token_count, experts_first)
    cap_second = capacity_for(token_count, experts_second)
    places_first = slot_places(route_first, experts_first, cap_first)
    places_second = slot_places(route_second, experts_second, cap_second)

    widened = tokens.astype(jnp.float32)
    normed_first = rms_normal(widened).astype(jnp.bfloat16)
    up_one, down_one, received_first, arriving_second = communicate(
        0,
        gathers=(up_first[0], down_first[0]),
        exchanges=(
            slotted(normed_first, places_first, experts_first, cap_first),
            slotted(cotangent, places_second, experts_second, cap_second),
        ),
    )
    pre_first, hidden_first = project_up(received_first, up_one)
    up_two, returned = communicate(
        1, gathers=(up_second[0],), exchanges=(project_down(hidden_first, down_one),)
    )
    middle = (widened + from_slots(returned, places_first, experts_first)).astype(jnp.bfloat16)
    middle_wide = middle.astype(jnp.float32)
    normed_second = rms_normal(middle_wide).astype(jnp.bfloat16)
    down_two, received_second = communicate(
        2,
        gathers=(down_second[0],),
        exchanges=(slotted(normed_second, places_second, experts_second, cap_second),),
    )
    pre_second, hidden_second = project_up(received_second, up_two)
    part_second = project_down(hidden_second, down_two)
    grad_up_two, grad_down_two, slot_grads = layer_gradients(
        arriving_second, received_second, pre_second, hidden_second, up_two, down_two
    )
    down_grad_second, coming_back = communicate(
        3, scatters=(grad_down_two,), exchanges=(slot_grads,)
    )
    grad_middle = grad_through_norm(
        cotangent, middle_wide, from_slots(coming_back, places_second, experts_second)
    )
    up_grad_second, arriving_first = communicate(
        4,
        scatters=(grad_up_two,),
        exchanges=(slotted(grad_middle, places_first, experts_first, cap_first),),
    )
    grad_up_one, grad_down_one, slot_grads = layer_gradients(
        arriving_first, received_first, pre_first, hidden_first, up_one, down_one
    )
    up_grad_first, down_grad_first, coming_back, returned = communicate(
        5, scatters=(grad_up_one, grad_down_one), exchanges=(slot_grads, part_second)
    )
    grad_tokens = grad_through_norm(
        grad_middle, widened, from_slots(coming_back, places_first, experts_first)
    )
    branch = from_slots(returned, places_second, experts_second)
    layer_out = (middle_wide + branch).astype(jnp.bfloat16)
    return (
        layer_out,
        grad_tokens,
        up_grad_first[None],
        down_grad_first[None],
        up_grad_second[None],
        down_grad_second[None],
    )


def solution(mesh):
    in_specs = (
        P(("dp", "expert"), None),
        P(("dp", "expert"), None),
        P(("dp", "expert"), None),
        P("expert", "dp", None),
        P("expert", "dp", None),
        P("expert", "dp", None),
        P("expert", "dp", None),
        P(("dp", "expert"), None),
    )
    out_specs = (
        P(("dp", "expert"), None),
        P(("dp", "expert"), None),
        P("expert", "dp", None),
        P("expert", "dp", None),
        P("expert", "dp", None),
        P("expert", "dp", None),
    )
    return jax.shard_map(local, mesh=mesh, in_specs=in_specs, out_specs=out_specs, check_vma=False)
```

```python
import functools

import jax
import jax.numpy as jnp
from jax import lax
from jax.experimental import pallas as pl
from jax.experimental.pallas import tpu as pltpu
from jax.sharding import PartitionSpec as P

epsilon = 1e-06


def rms_normal(widened):
    return widened * lax.rsqrt(jnp.mean(widened * widened, axis=-1, keepdims=True) + epsilon)


def gelu_slope(pre_gelu):
    _, pullback = jax.vjp(jax.nn.gelu, pre_gelu)
    return pullback(jnp.ones_like(pre_gelu))[0]


def slot_places(route_ids, experts, capacity):
    expert_ids = route_ids[:, 0]
    onehot = (expert_ids[:, None] == jnp.arange(experts, dtype=jnp.int32)[None, :]).astype(
        jnp.int32
    )
    earlier = jnp.cumsum(onehot, axis=0) - onehot
    return expert_ids * capacity + jnp.sum(earlier * onehot, axis=1)


def to_slots(token_rows, places, slot_count):
    onehot_table = (places[None, :] == jnp.arange(slot_count, dtype=jnp.int32)[:, None]).astype(
        token_rows.dtype
    )
    return jnp.dot(onehot_table, token_rows, preferred_element_type=jnp.float32).astype(
        token_rows.dtype
    )


def from_slots(returned, places, experts):
    group_size = returned.shape[0] // experts
    feature_count = returned.shape[2]
    summed = (
        returned.reshape(experts, group_size, returned.shape[1], feature_count)
        .astype(jnp.float32)
        .sum(axis=1)
    )
    summed = summed.reshape(-1, feature_count)
    onehot_table = (
        places[:, None] == jnp.arange(summed.shape[0], dtype=jnp.int32)[None, :]
    ).astype(jnp.float32)
    return jnp.dot(
        onehot_table, summed, precision=lax.Precision.HIGHEST, preferred_element_type=jnp.float32
    )


def moe_forward(token_rows, route_ids, weights, experts, capacity):
    up_full, down_full = weights
    group_size = lax.axis_size("expert") // experts
    places = slot_places(route_ids, experts, capacity)
    widened = token_rows.astype(jnp.float32)
    normed = rms_normal(widened).astype(jnp.bfloat16)
    slot_rows = to_slots(normed, places, experts * capacity).reshape(experts, capacity, -1)
    outgoing = jnp.repeat(slot_rows, group_size, axis=0)
    received = lax.all_to_all(outgoing, "expert", split_axis=0, concat_axis=0, tiled=True)
    pre_gelu = jnp.einsum("skd,dh->skh", received, up_full, preferred_element_type=jnp.float32)
    hidden = jax.nn.gelu(pre_gelu).astype(jnp.bfloat16)
    partial_out = jnp.einsum(
        "skh,hd->skd", hidden, down_full, preferred_element_type=jnp.float32
    ).astype(jnp.bfloat16)
    returned = lax.all_to_all(partial_out, "expert", split_axis=0, concat_axis=0, tiled=True)
    returned, received, pre_gelu, hidden = (returned, received, pre_gelu, hidden)
    branch = from_slots(returned, places, experts)
    layer_out = (widened + branch).astype(jnp.bfloat16)
    return (layer_out, (widened, places, received, pre_gelu, hidden))


def moe_backward(upstream, saved, weights, experts, capacity):
    up_full, down_full = weights
    widened, places, received, pre_gelu, hidden = saved
    group_size = lax.axis_size("expert") // experts
    slot_rows = to_slots(upstream, places, experts * capacity).reshape(experts, capacity, -1)
    outgoing = jnp.repeat(slot_rows, group_size, axis=0)
    arriving = lax.all_to_all(outgoing, "expert", split_axis=0, concat_axis=0, tiled=True)
    grad_hidden = jnp.einsum("skd,hd->skh", arriving, down_full, preferred_element_type=jnp.float32)
    grad_pre = (grad_hidden * gelu_slope(pre_gelu)).astype(jnp.bfloat16)
    grad_down = jnp.einsum("skh,skd->hd", hidden, arriving, preferred_element_type=jnp.float32)
    grad_up = jnp.einsum("skd,skh->dh", received, grad_pre, preferred_element_type=jnp.float32)
    grad_slots = jnp.einsum(
        "skh,dh->skd", grad_pre, up_full, preferred_element_type=jnp.float32
    ).astype(jnp.bfloat16)
    coming_back = lax.all_to_all(grad_slots, "expert", split_axis=0, concat_axis=0, tiled=True)
    grad_normed = from_slots(coming_back, places, experts)
    _, pullback = jax.vjp(rms_normal, widened)
    grad_input = (upstream.astype(jnp.float32) + pullback(grad_normed)[0]).astype(jnp.bfloat16)
    return (grad_input, grad_up, grad_down)


def fetch_layer(up_shard, down_shard):
    up_full, down_full = (
        lax.all_gather(up_shard, "dp", axis=1, tiled=True),
        lax.all_gather(down_shard, "dp", axis=1, tiled=True),
    )
    return (up_full[0], down_full[0])


def capacity_for(token_count, experts):
    return min(token_count, (token_count * 17 + 16 * experts - 1) // (16 * experts))


def local_plain(
    tokens, route_first, route_second, up_first, down_first, up_second, down_second, cotangent
):
    expert_devices = lax.axis_size("expert")
    token_count = tokens.shape[0]
    experts_first = max(expert_devices // 4, 2)
    experts_second = max(expert_devices // 2, 2)
    cap_first = capacity_for(token_count, experts_first)
    cap_second = capacity_for(token_count, experts_second)
    first_weights = fetch_layer(up_first, down_first)
    middle, first_saved = moe_forward(tokens, route_first, first_weights, experts_first, cap_first)
    second_weights = fetch_layer(up_second, down_second)
    layer_out, second_saved = moe_forward(
        middle, route_second, second_weights, experts_second, cap_second
    )
    grad_middle, up_grad_second, down_grad_second = moe_backward(
        cotangent, second_saved, second_weights, experts_second, cap_second
    )
    grad_tokens, up_grad_first, down_grad_first = moe_backward(
        grad_middle, first_saved, first_weights, experts_first, cap_first
    )
    reduced_all = (
        lax.psum_scatter(
            up_grad_first.astype(jnp.bfloat16), "dp", scatter_dimension=0, tiled=True
        ).astype(jnp.float32),
        lax.psum_scatter(
            down_grad_first.astype(jnp.bfloat16), "dp", scatter_dimension=0, tiled=True
        ).astype(jnp.float32),
        lax.psum_scatter(
            up_grad_second.astype(jnp.bfloat16), "dp", scatter_dimension=0, tiled=True
        ).astype(jnp.float32),
        lax.psum_scatter(
            down_grad_second.astype(jnp.bfloat16), "dp", scatter_dimension=0, tiled=True
        ).astype(jnp.float32),
    )
    reduced_first = (reduced_all[0][None], reduced_all[1][None])
    reduced_second = (reduced_all[2][None], reduced_all[3][None])
    return (
        layer_out,
        grad_tokens,
        reduced_first[0],
        reduced_first[1],
        reduced_second[0],
        reduced_second[1],
    )


VMEM_LIMIT = 56 * 1024 * 1024


def block_tables(route, experts, capacity):
    count = route.shape[0]
    lanes = lax.broadcasted_iota(jnp.int32, (count, count), 1)
    rows = lax.broadcasted_iota(jnp.int32, (count, count), 0)
    onehot = jnp.where(lanes == route, 1.0, 0.0)
    below = jnp.where(lanes < rows, 1.0, 0.0)
    earlier = jnp.dot(
        below.astype(jnp.bfloat16), onehot.astype(jnp.bfloat16), preferred_element_type=jnp.float32
    )
    place = jnp.sum(earlier * onehot, axis=1, keepdims=True).astype(jnp.int32)
    slots = lax.broadcasted_iota(jnp.int32, (count, capacity), 1)
    hit = jnp.where(slots == place, 1.0, 0.0)
    return [
        (hit * jnp.where(route == expert, 1.0, 0.0)).astype(jnp.bfloat16)
        for expert in range(experts)
    ]


def fill_slots(target, tables, token_rows):
    for expert, table in enumerate(tables):
        target[expert] = lax.dot_general(
            table, token_rows, (((0,), (0,)), ((), ())), preferred_element_type=jnp.float32
        ).astype(target.dtype)


def pick_up(parts, tables):
    group_size = parts.shape[0] // len(tables)
    total = None
    for part in range(parts.shape[0]):
        picked = jnp.dot(
            tables[part // group_size], parts[part], preferred_element_type=jnp.float32
        )
        total = picked if total is None else total + picked
    return total


def add_norm_pullback(upstream, widened, grad_normed):
    scale = lax.rsqrt(jnp.mean(widened * widened, axis=-1, keepdims=True) + epsilon)
    along = jnp.mean(grad_normed * widened, axis=-1, keepdims=True)
    pulled = scale * grad_normed - widened * (scale * scale * scale * along)
    return (upstream.astype(jnp.float32) + pulled).astype(jnp.bfloat16)


def stage_kernel(stage, experts_first, experts_second, capacities, *refs):
    refs = list(refs)

    def take(count):
        taken = refs[:count]
        del refs[:count]
        return taken

    cap_first, cap_second = capacities
    gathering = stage < 2
    shards, grads, fulls, sums, scatter_scratch = [], [], [], [], []
    if gathering:
        shards = take(2)
    else:
        grads = take(2)
    if stage == 0:
        route_first, route_second, tokens, cotangent = take(4)
        *fulls, received, arriving, slots_one, slots_two = take(6)
    elif stage == 1:
        route_first, route_second, tokens, parts = take(4)
        *fulls, received, middle, back, slots_one = take(6)
    elif stage == 2:
        route_first, route_second, cotangent, middle, parts = take(5)
        *sums, arriving, grad_middle, back, slots_one = take(6)
    else:
        route_first, route_second, tokens, middle, grad_middle, parts, parts_second = take(7)
        *sums, grad_tokens, layer_out, back, back_second = take(6)
    if not gathering:
        scatter_scratch = [take(8) for _ in grads]
    gather_rows = [shard.shape[0] for shard in shards]
    scatter_rows = [total.shape[0] for total in sums]
    send_sems, recv_sems, local_sems = take(3)
    used = [0, 0]

    dp = lax.axis_index("dp")
    z = lax.axis_index("expert")
    z_count = lax.axis_size("expert")
    core = lax.rem(dp, 2)
    x_bit = lax.rem(lax.div(dp, 2), 2)
    y_bit = lax.div(dp, 4)
    twin = dp + 1 - 2 * core
    x_side = dp + 2 - 4 * x_bit
    y_side = dp + 4 - 8 * y_bit
    diagonal = x_side + 4 - 8 * y_bit

    barrier = pltpu.get_barrier_semaphore()
    peers = 0
    for side in (twin, x_side, y_side):
        pl.semaphore_signal(
            barrier, inc=1, device_id=(side, z), device_id_type=pl.DeviceIdType.MESH
        )
        peers += 1
    for step in range(1, z_count):
        pl.semaphore_signal(
            barrier,
            inc=1,
            device_id=(dp, lax.rem(z + step, z_count)),
            device_id_type=pl.DeviceIdType.MESH,
        )
        peers += 1
    pl.semaphore_wait(barrier, peers)

    def send(source, target, to_dp, to_z):
        index = used[0]
        used[0] += 1
        copy = pltpu.make_async_remote_copy(
            src_ref=source,
            dst_ref=target,
            send_sem=send_sems.at[index],
            recv_sem=recv_sems.at[index],
            device_id=(to_dp, to_z),
            device_id_type=pl.DeviceIdType.MESH,
        )
        copy.start()
        return copy

    def keep(source, target):
        index = used[1]
        used[1] += 1
        copy = pltpu.make_async_copy(source, target, local_sems.at[index])
        copy.start()
        return copy

    remote, local = [], []
    swaps = []
    def rows_of(ref, owner, rows, start=0, count=None):
        offset = pl.multiple_of(owner * rows + start, rows if count is None else count)
        return ref.at[pl.ds(offset, rows if count is None else count), :]

    def wide(ref):
        return ref[...].astype(jnp.float32)

    def exchange(source, target):
        slots = source.shape[0]
        copies = []
        for step in range(1, z_count):
            to_z = lax.rem(z + step, z_count)
            slot = lax.div(to_z * slots, z_count)
            copies.append(send(source.at[slot], target.at[z], dp, to_z))
        copies.append(keep(source.at[lax.div(z * slots, z_count)], target.at[z]))
        return copies

    def finish(copies):
        for copy in copies:
            copy.wait()

    for grad, rows, scratch in zip(grads, scatter_rows, scatter_scratch):
        from_twin = scratch[0]
        swap = []
        for slot, owner in enumerate((diagonal, x_side, y_side, dp)):
            theirs = owner + 1 - 2 * core
            part = grad.at[pl.ds(pl.multiple_of(theirs * rows, rows), rows), :]
            swap.append(send(part, from_twin.at[slot], twin, z))
        swaps.append(swap)

    if stage > 0:
        returning = exchange(parts, back)
    if stage == 3:
        returning_second = exchange(parts_second, back_second)

    firsts = []
    for shard, full, rows in zip(shards, fulls, gather_rows):
        mine = rows_of(full, dp, rows)
        firsts.append((send(shard, mine, x_side, z), send(shard, mine, y_side, z)))
        remote.append(send(shard, mine, twin, z))
        local.append(keep(shard, mine))

    halves = []
    for grad, rows, scratch, swap in zip(grads, scatter_rows, scatter_scratch, swaps):
        from_twin, to_diagonal, to_x, to_y, via_x, via_y, from_x, from_y = scratch
        half = rows // 2
        swap[0].wait_recv()
        to_diagonal[...] = (
            wide(rows_of(grad, diagonal, rows)) + wide(from_twin.at[0])
        ).astype(jnp.bfloat16)
        swap[1].wait_recv()
        to_x[...] = (wide(rows_of(grad, x_side, rows)) + wide(from_twin.at[1])).astype(
            jnp.bfloat16
        )
        low, high = pl.ds(0, half), pl.ds(half, half)
        relay_x = send(to_diagonal.at[low, :], via_x, x_side, z)
        relay_y = send(to_diagonal.at[high, :], via_y, y_side, z)
        swap[2].wait_recv()
        to_y[...] = (wide(rows_of(grad, y_side, rows)) + wide(from_twin.at[2])).astype(
            jnp.bfloat16
        )
        direct_x = send(to_x.at[low, :], from_x.at[low, :], x_side, z)
        direct_y = send(to_y.at[high, :], from_y.at[high, :], y_side, z)
        swap[3].wait_recv()
        halves.append((relay_x, relay_y, direct_x, direct_y))
    first_tables = block_tables(route_first[...], experts_first, cap_first)
    second_tables = block_tables(route_second[...], experts_second, cap_second)
    if stage == 0:
        normed = rms_normal(wide(tokens)).astype(jnp.bfloat16)
        fill_slots(slots_one, first_tables, normed)
        fill_slots(slots_two, second_tables, cotangent[...])
        onward = exchange(slots_one, received) + exchange(slots_two, arriving)
    elif stage == 1:
        finish(returning)
        middle_rows = (wide(tokens) + pick_up(back, first_tables)).astype(jnp.bfloat16)
        normed = rms_normal(middle_rows.astype(jnp.float32)).astype(jnp.bfloat16)
        fill_slots(slots_one, second_tables, normed)
        middle[...] = middle_rows
        onward = exchange(slots_one, received)
    elif stage == 2:
        finish(returning)
        grad_rows = add_norm_pullback(
            cotangent[...], wide(middle), pick_up(back, second_tables)
        )
        fill_slots(slots_one, first_tables, grad_rows)
        grad_middle[...] = grad_rows
        onward = exchange(slots_one, arriving)
    else:
        onward = []

    diagonals = []
    for full, rows, (along_x, along_y) in zip(fulls, gather_rows, firsts):
        half = rows // 2
        along_x.wait_recv()
        part = rows_of(full, x_side, rows, 0, half)
        lower = send(part, part, y_side, z)
        part = rows_of(full, x_side, rows)
        remote.append(send(part, part, twin, z))
        along_y.wait_recv()
        part = rows_of(full, y_side, rows, half, half)
        upper = send(part, part, x_side, z)
        part = rows_of(full, y_side, rows)
        remote.append(send(part, part, twin, z))
        along_x.wait_send()
        along_y.wait_send()
        diagonals.append((lower, upper))
    for full, rows, (lower, upper) in zip(fulls, gather_rows, diagonals):
        half = rows // 2
        lower.wait_recv()
        part = rows_of(full, diagonal, rows, 0, half)
        remote.append(send(part, part, twin, z))
        upper.wait_recv()
        part = rows_of(full, diagonal, rows, half, half)
        remote.append(send(part, part, twin, z))
        lower.wait_send()
        upper.wait_send()

    finals = []
    for rows, scratch, (relay_x, relay_y, direct_x, direct_y) in zip(
        scatter_rows, scatter_scratch, halves
    ):
        from_twin, to_diagonal, to_x, to_y, via_x, via_y, from_x, from_y = scratch
        half = rows // 2
        low, high = pl.ds(0, half), pl.ds(half, half)
        relay_y.wait_recv()
        to_x[high, :] = (wide(to_x.at[high, :]) + wide(via_y)).astype(jnp.bfloat16)
        relay_x.wait_recv()
        to_y[low, :] = (wide(to_y.at[low, :]) + wide(via_x)).astype(jnp.bfloat16)
        last_x = send(to_x.at[high, :], from_x.at[high, :], x_side, z)
        last_y = send(to_y.at[low, :], from_y.at[low, :], y_side, z)
        finals.append((last_x, last_y))
    if stage == 3:
        finish(returning)
        grad_tokens[...] = add_norm_pullback(
            grad_middle[...], wide(tokens), pick_up(back, first_tables)
        )
        finish(returning_second)
        layer_out[...] = (wide(middle) + pick_up(back_second, second_tables)).astype(jnp.bfloat16)
    for grad, total, rows, scratch, swap, pieces, last in zip(
        grads, sums, scatter_rows, scatter_scratch, swaps, halves, finals
    ):
        from_twin, to_diagonal, to_x, to_y, via_x, via_y, from_x, from_y = scratch
        for copy in pieces[2:] + last:
            copy.wait_recv()
        total[...] = (
            wide(rows_of(grad, dp, rows)) + wide(from_twin.at[3]) + wide(from_x) + wide(from_y)
        )
        for copy in tuple(swap) + pieces + last:
            copy.wait_send()
    finish(onward)
    finish(remote)
    finish(local)


def run_stage(stage, experts_first, experts_second, capacities, matrices, others, outs, slotted):
    ways = lax.axis_size("dp")
    z_count = lax.axis_size("expert")
    shapes, out_specs = [], []
    scratch = [pltpu.VMEM(shape, jnp.bfloat16) for shape in slotted]
    for matrix in matrices:
        if stage < 2:
            shapes.append(
                jax.ShapeDtypeStruct((ways * matrix.shape[0], matrix.shape[1]), matrix.dtype)
            )
            out_specs.append(pl.BlockSpec(memory_space=pl.ANY))
        else:
            rows, columns = matrix.shape[0] // ways, matrix.shape[1]
            shapes.append(jax.ShapeDtypeStruct((rows, columns), jnp.float32))
            out_specs.append(pl.BlockSpec(memory_space=pltpu.VMEM))
            scratch.append(pltpu.VMEM((4, rows, columns), matrix.dtype))
            for height in (rows, rows, rows, rows // 2, rows // 2, rows, rows):
                scratch.append(pltpu.VMEM((height, columns), matrix.dtype))
    for shape, in_vmem in outs:
        shapes.append(jax.ShapeDtypeStruct(shape, jnp.bfloat16))
        out_specs.append(pl.BlockSpec(memory_space=pltpu.VMEM if in_vmem else pl.ANY))
    copies = 10 * len(matrices) + 2 * (z_count - 1)
    scratch += [
        pltpu.SemaphoreType.DMA((copies,)),
        pltpu.SemaphoreType.DMA((copies,)),
        pltpu.SemaphoreType.DMA((len(matrices) + 2,)),
    ]
    inputs = (*matrices, *others)
    return pl.pallas_call(
        functools.partial(stage_kernel, stage, experts_first, experts_second, capacities),
        out_shape=tuple(shapes),
        in_specs=[pl.BlockSpec(memory_space=pltpu.VMEM)] * len(inputs),
        out_specs=tuple(out_specs),
        scratch_shapes=scratch,
        compiler_params=pltpu.CompilerParams(
            collective_id=stage, has_side_effects=True, vmem_limit_bytes=VMEM_LIMIT
        ),
        name="stage_%d" % stage,
    )(*inputs)


def project_up(received, up_full):
    pre_gelu = jnp.einsum("skd,dh->skh", received, up_full, preferred_element_type=jnp.float32)
    return pre_gelu, jax.nn.gelu(pre_gelu).astype(jnp.bfloat16)


def project_down(hidden, down_full):
    return jnp.einsum("skh,hd->skd", hidden, down_full, preferred_element_type=jnp.float32).astype(
        jnp.bfloat16
    )


def layer_gradients(arriving, received, pre_gelu, hidden, up_full, down_full):
    grad_hidden = jnp.einsum("skd,hd->skh", arriving, down_full, preferred_element_type=jnp.float32)
    grad_pre = (grad_hidden * gelu_slope(pre_gelu)).astype(jnp.bfloat16)
    grad_down = jnp.einsum("skh,skd->hd", hidden, arriving, preferred_element_type=jnp.float32)
    grad_up = jnp.einsum("skd,skh->dh", received, grad_pre, preferred_element_type=jnp.float32)
    grad_slots = jnp.einsum(
        "skh,dh->skd", grad_pre, up_full, preferred_element_type=jnp.float32
    ).astype(jnp.bfloat16)
    return grad_up.astype(jnp.bfloat16), grad_down.astype(jnp.bfloat16), grad_slots


def local(
    tokens, route_first, route_second, up_first, down_first, up_second, down_second, cotangent
):
    arguments = (
        tokens,
        route_first,
        route_second,
        up_first,
        down_first,
        up_second,
        down_second,
        cotangent,
    )
    z_count = lax.axis_size("expert")
    if lax.axis_size("dp") != 8:
        return local_plain(*arguments)
    rows, width = tokens.shape
    experts_first = max(z_count // 4, 2)
    experts_second = max(z_count // 2, 2)
    cap_first = -(-capacity_for(rows, experts_first) // 8) * 8
    cap_second = -(-capacity_for(rows, experts_second) // 8) * 8
    sizes = (experts_first, experts_second, (cap_first, cap_second))
    outgoing_first = (experts_first, cap_first, width)
    outgoing_second = (experts_second, cap_second, width)
    incoming_first = (z_count, cap_first, width)
    incoming_second = (z_count, cap_second, width)

    up_one, down_one, received_first, arriving_second = run_stage(
        0,
        *sizes,
        (up_first[0], down_first[0]),
        (route_first, route_second, tokens, cotangent),
        ((incoming_first, False), (incoming_second, False)),
        (outgoing_first, outgoing_second),
    )
    pre_first, hidden_first = project_up(received_first, up_one)
    up_two, down_two, received_second, middle = run_stage(
        1,
        *sizes,
        (up_second[0], down_second[0]),
        (route_first, route_second, tokens, project_down(hidden_first, down_one)),
        ((incoming_second, False), (tokens.shape, True)),
        (incoming_first, outgoing_second),
    )
    pre_second, hidden_second = project_up(received_second, up_two)
    part_second = project_down(hidden_second, down_two)
    grad_up_two, grad_down_two, slot_grads = layer_gradients(
        arriving_second, received_second, pre_second, hidden_second, up_two, down_two
    )
    up_grad_second, down_grad_second, arriving_first, grad_middle = run_stage(
        2,
        *sizes,
        (grad_up_two, grad_down_two),
        (route_first, route_second, cotangent, middle, slot_grads),
        ((incoming_first, False), (tokens.shape, True)),
        (incoming_second, outgoing_first),
    )
    grad_up_one, grad_down_one, slot_grads = layer_gradients(
        arriving_first, received_first, pre_first, hidden_first, up_one, down_one
    )
    up_grad_first, down_grad_first, grad_tokens, layer_out = run_stage(
        3,
        *sizes,
        (grad_up_one, grad_down_one),
        (route_first, route_second, tokens, middle, grad_middle, slot_grads, part_second),
        ((tokens.shape, True), (tokens.shape, True)),
        (incoming_first, incoming_second),
    )
    return (
        layer_out,
        grad_tokens,
        up_grad_first[None],
        down_grad_first[None],
        up_grad_second[None],
        down_grad_second[None],
    )


def solution(mesh):
    in_specs = (
        P(("dp", "expert"), None),
        P(("dp", "expert"), None),
        P(("dp", "expert"), None),
        P("expert", "dp", None),
        P("expert", "dp", None),
        P("expert", "dp", None),
        P("expert", "dp", None),
        P(("dp", "expert"), None),
    )
    out_specs = (
        P(("dp", "expert"), None),
        P(("dp", "expert"), None),
        P("expert", "dp", None),
        P("expert", "dp", None),
        P("expert", "dp", None),
        P("expert", "dp", None),
    )
    return jax.shard_map(local, mesh=mesh, in_specs=in_specs, out_specs=out_specs, check_vma=False)
```
